8 devices in a mesh: dp: 1 (over z), pp: 2 (over y), tp: 4 (over x, core).
Axes of the slice: x: 2, y: 2, z: 1, core: 2. Of those that a mesh axis runs over, the one named last changes fastest.
Arguments:
- x_in: bfloat16 [12, 512, 4096], P('dp', 'tp')
- ln_gain: bfloat16 [2, 2, 4096], P(None, 'pp')
- w_in: bfloat16 [2, 2, 4096, 16384], P(None, 'pp', None, 'tp')
- w_out: bfloat16 [2, 2, 16384, 4096], P(None, 'pp', 'tp')
Outputs:
- output: bfloat16 [12, 512, 4096], P(('dp', 'pp'), 'tp')
All inputs are finite; a program needn't handle non-finite values.
Results may differ from the reference program's by a relative error of at most 0.0177071.
Values are sent between devices in bfloat16 or wider.
A program may use at most 1 GiB of HBM per device.

```python
import jax
import jax.numpy as jnp
from jax import lax

MODEL_DIM = 4096
FFN_DIM = 16384
STAGES = 2
TP_RANKS = 4
MICRO_BATCHES = 12
SEQ_TOKENS = 512

NORM_EPS = 1e-5
SHARD_FFN = FFN_DIM // TP_RANKS
BLOCK_COUNT = 2 * STAGES


def setup_inputs(seed: int = 0, part: int = 0) -> dict:
    base_key = jax.random.key(seed)
    act_key = jax.random.fold_in(jax.random.fold_in(base_key, 1), part)
    gain_key, first_key, second_key = jax.random.split(jax.random.fold_in(base_key, 2), 3)
    x_vals = jax.random.normal(act_key, (MICRO_BATCHES, SEQ_TOKENS, MODEL_DIM), jnp.float32)
    gain_vals = 1.0 + 0.25 * jax.random.normal(gain_key, (2, STAGES, MODEL_DIM), jnp.float32)
    first_vals = jax.random.normal(first_key, (2, STAGES, MODEL_DIM, FFN_DIM), jnp.float32) * MODEL_DIM ** -0.5
    second_vals = jax.random.normal(second_key, (2, STAGES, FFN_DIM, MODEL_DIM), jnp.float32) * FFN_DIM ** -0.5
    return {"x_in": x_vals.astype(jnp.bfloat16), "ln_gain": gain_vals.astype(jnp.bfloat16), "w_in": first_vals.astype(jnp.bfloat16), "w_out": second_vals.astype(jnp.bfloat16)}


def mlp_block(resid, gain_vec, w_first, w_second):
    resid_f = resid.astype(jnp.float32)
    row_mean = jnp.mean(resid_f, axis=-1, keepdims=True)
    centred = resid_f - row_mean
    row_var = jnp.mean(centred * centred, axis=-1, keepdims=True)
    normed = (centred * lax.rsqrt(row_var + NORM_EPS) * gain_vec.astype(jnp.float32)).astype(jnp.bfloat16)
    hidden = jax.nn.gelu(jnp.dot(normed, w_first, preferred_element_type=jnp.float32)).astype(jnp.bfloat16)
    hidden_shards = hidden.reshape(SEQ_TOKENS, TP_RANKS, SHARD_FFN).transpose(1, 0, 2)
    w_shards = w_second.reshape(TP_RANKS, SHARD_FFN, MODEL_DIM)

    def add_shard(acc_sum, shard_pair):
        h_shard, w_shard = shard_pair
        part_prod = jnp.dot(h_shard, w_shard, preferred_element_type=jnp.float32)
        return acc_sum + part_prod.astype(jnp.bfloat16).astype(jnp.float32), None

    mlp_sum, _ = lax.scan(add_shard, jnp.zeros((SEQ_TOKENS, MODEL_DIM), jnp.float32), (hidden_shards, w_shards))
    return (resid_f + mlp_sum).astype(jnp.bfloat16)


def reference(x_in, ln_gain, w_in, w_out):
    gain_rows = ln_gain.reshape(BLOCK_COUNT, MODEL_DIM)
    firsts = w_in.reshape(BLOCK_COUNT, MODEL_DIM, FFN_DIM)
    seconds = w_out.reshape(BLOCK_COUNT, FFN_DIM, MODEL_DIM)

    def one_block(resid, block_w):
        gain_vec, w_first, w_second = block_w
        return mlp_block(resid, gain_vec, w_first, w_second), None

    def one_micro(micro_x):
        result, _ = lax.scan(one_block, micro_x, (gain_rows, firsts, seconds))
        return result

    return lax.map(one_micro, x_in)
```

```python
import jax
import jax.numpy as jnp
from jax import lax
from jax.experimental import pallas as pl
from jax.experimental.pallas import tpu as pltpu
from jax.sharding import PartitionSpec as P

NORM_EPS = 1e-5
LAG = 4
TILE = 512


def layer_norm(resid, gain_vec):
    resid_f = resid.astype(jnp.float32)
    row_mean = jnp.mean(resid_f, axis=-1, keepdims=True)
    centred = resid_f - row_mean
    row_var = jnp.mean(centred * centred, axis=-1, keepdims=True)
    return (centred * lax.rsqrt(row_var + NORM_EPS) * gain_vec.astype(jnp.float32)).astype(jnp.bfloat16)


def norm_kernel(sel_ref, a_ref, b_ref, gain_ref, y_ref, h_ref):
    @pl.when(sel_ref[0] == 0)
    def _():
        y_ref[...] = a_ref[...]

    @pl.when(sel_ref[0] != 0)
    def _():
        y_ref[...] = b_ref[...]

    gain = jnp.where(sel_ref[1] == 0, gain_ref[0].astype(jnp.float32), gain_ref[1].astype(jnp.float32))
    h_ref[...] = layer_norm(y_ref[...], gain)


def select_norm(sel, a, b, gains):
    rows, dim = a.shape
    step = 32
    spec = pl.BlockSpec((step, dim), lambda i, s: (i, 0))
    return pl.pallas_call(
        norm_kernel,
        out_shape=[jax.ShapeDtypeStruct((rows, dim), jnp.bfloat16)] * 2,
        grid_spec=pltpu.PrefetchScalarGridSpec(
            num_scalar_prefetch=1,
            grid=(rows // step,),
            in_specs=[spec, spec, pl.BlockSpec((2, 1, dim), lambda i, s: (0, 0, 0))],
            out_specs=[spec, spec],
        ),
        compiler_params=pltpu.CompilerParams(vmem_limit_bytes=8 * 2**20),
        cost_estimate=pl.CostEstimate(flops=10**9, bytes_accessed=5 * 2**20, transcendentals=0),
        name="select_norm",
    )(sel, a, b, gains)


def up_kernel(v_ref, own, far, sib, w_ref, o_ref, h, sem):
    rows = own.shape[0]

    @pl.when(pl.program_id(0) == 0)
    def _():
        copies = [
            pltpu.make_async_copy(own, h.at[pl.ds(0, rows)], sem.at[0]),
            pltpu.make_async_copy(far, h.at[pl.ds(rows, rows)], sem.at[1]),
            pltpu.make_async_copy(sib, h.at[pl.ds(2 * rows, 2 * rows)], sem.at[2]),
        ]
        for c in copies:
            c.start()
        for c in copies:
            c.wait()

    o_ref[...] = jax.nn.gelu(jnp.dot(h[...], w_ref[...], preferred_element_type=jnp.float32)).astype(jnp.bfloat16)


def up_project(v, own, far, sib, w):
    rows, dim, width = 4 * own.shape[0], w.shape[2], w.shape[3]
    return pl.pallas_call(
        up_kernel,
        out_shape=jax.ShapeDtypeStruct((rows, width), jnp.bfloat16),
        grid_spec=pltpu.PrefetchScalarGridSpec(
            num_scalar_prefetch=1,
            grid=(width // TILE,),
            in_specs=[pl.BlockSpec(memory_space=pl.ANY)] * 3
            + [pl.BlockSpec((None, None, dim, TILE), lambda j, v: (v[0], 0, 0, j))],
            out_specs=pl.BlockSpec((rows, TILE), lambda j, v: (0, j)),
            scratch_shapes=[pltpu.VMEM((rows, dim), jnp.bfloat16), pltpu.SemaphoreType.DMA((3,))],
        ),
        compiler_params=pltpu.CompilerParams(vmem_limit_bytes=24 * 2**20),
        cost_estimate=pl.CostEstimate(flops=2 * rows * dim * width, bytes_accessed=40 * 2**20, transcendentals=rows * width),
        name="up_project",
    )(v, own, far, sib, w)


def down_kernel(v_ref, a_ref, w_ref, keep, send):
    part = jnp.dot(a_ref[...], w_ref[...], preferred_element_type=jnp.float32).astype(jnp.bfloat16)
    half = part.shape[0] // 2
    keep[...] = part[:half]
    send[...] = part[half:]


def down_project(v, a, w):
    rows, width, dim = a.shape[0], w.shape[2], w.shape[3]
    return pl.pallas_call(
        down_kernel,
        out_shape=[jax.ShapeDtypeStruct((rows // 2, dim), jnp.bfloat16)] * 2,
        grid_spec=pltpu.PrefetchScalarGridSpec(
            num_scalar_prefetch=1,
            grid=(dim // TILE,),
            in_specs=[
                pl.BlockSpec((rows, width), lambda j, v: (0, 0)),
                pl.BlockSpec((None, None, width, TILE), lambda j, v: (v[0], 0, 0, j)),
            ],
            out_specs=[pl.BlockSpec((rows // 2, TILE), lambda j, v: (0, j))] * 2,
        ),
        compiler_params=pltpu.CompilerParams(vmem_limit_bytes=24 * 2**20),
        cost_estimate=pl.CostEstimate(flops=2 * rows * dim * width, bytes_accessed=40 * 2**20, transcendentals=0),
        name="down_project",
    )(v, a, w)


def solution(mesh):
    stages = mesh.shape["pp"]
    ranks = mesh.shape["tp"]
    assert stages == 2 and ranks == 4
    core_perm = [(r, r ^ 1) for r in range(ranks)]
    chip_perm = [(r, r ^ 2) for r in range(ranks)]
    stage_perm = [(0, 1), (1, 0)]

    def per_device(x_loc, gain_loc, w_in_loc, w_out_loc):
        micro, tok = x_loc.shape[0], x_loc.shape[1]
        items = 2 * micro
        ticks = items + LAG
        stage = lax.axis_index("pp")
        first = stage == 0
        f32 = jnp.float32

        def virt(t):
            v0 = min(max(t, 0), items - 1) // micro
            v1 = min(max(t - LAG, 0), items - 1) // micro
            return jnp.where(first, v0, v1).astype(jnp.int32)

        shard, norm, far, sib = {}, {}, {}, {}
        keep, got, new, recv = {}, {}, {}, {}

        def make_norm(t):
            if t >= ticks:
                return
            in0 = x_loc[t] if t < micro else recv.get(t - micro + LAG)
            in1 = recv.get(t - LAG)
            a = in1 if in0 is None else in0
            b = in0 if in1 is None else in1
            sel = jnp.stack([stage.astype(jnp.int32), virt(t)])
            shard[t], norm[t] = select_norm(sel, a, b, gain_loc)

        def gather_chip(t):
            if t < ticks:
                far[t] = lax.ppermute(norm[t], "tp", chip_perm)

        def gather_core(t):
            if t < ticks:
                sib[t] = lax.ppermute(jnp.concatenate([norm[t], far[t]], axis=0), "tp", core_perm)

        def scatter_chip(t):
            k, g = keep[t], got[t]
            out = (k[tok:].astype(f32) + g[tok:].astype(f32)).astype(jnp.bfloat16)
            return lax.ppermute(out, "tp", chip_perm), out

        def finish(t, other):
            k, g = keep[t], got[t]
            total = k[:tok].astype(f32) + g[:tok].astype(f32) + other.astype(f32)
            return (shard[t].astype(f32) + total).astype(jnp.bfloat16)

        def tie(main, extras):
            keys = [(d, k) for d, k in extras if k in d]
            vals = lax.optimization_barrier((main, *[d[k] for d, k in keys]))
            for (d, k), val in zip(keys, vals[1:]):
                d[k] = val
            return vals[0]

        other = {}
        for t in (0, 1):
            make_norm(t)
            gather_chip(t)
        gather_core(0)
        for t in range(ticks):
            v = virt(t).reshape(1)
            if t >= 1:
                gather_core(t)
            hidden = up_project(v, norm[t], far[t], sib[t], w_in_loc)
            hidden = tie(hidden, [(got, t - 1), (recv, t - 2), (far, t + 1)])
            if t >= 1:
                other[t - 1], sent = scatter_chip(t - 1)
            make_norm(t + 2)
            keep[t], send = down_project(v, hidden, w_out_loc)
            send = tie(send, [(other, t - 1), (norm, t + 2)])
            if t >= 1:
                new[t - 1] = finish(t - 1, other[t - 1])
                recv[t - 1] = lax.ppermute(new[t - 1], "pp", stage_perm)
            gather_chip(t + 2)
            got[t] = lax.ppermute(send, "tp", core_perm)
        t = ticks - 1
        other[t], _ = scatter_chip(t)
        new[t] = finish(t, other[t])

        half = micro // stages
        outs = []
        for k in range(half):
            outs.append(jnp.where(first, recv[micro + k + LAG], new[micro + half + k + LAG]))
        return jnp.stack(outs, axis=0)

    return jax.shard_map(per_device, mesh=mesh, in_specs=(P("dp", "tp", None), P(None, "pp", None), P(None, "pp", None, "tp"), P(None, "pp", "tp", None)), out_specs=P(("dp", "pp"), "tp", None), check_vma=False)
```

```python
import functools

import jax
import jax.numpy as jnp
from jax import lax
from jax.experimental import pallas as pl
from jax.experimental.pallas import tpu as pltpu
from jax.sharding import PartitionSpec as P

NORM_EPS = 1e-5
LAG = 3
TILE = 512
SLOTS = 3
F32 = jnp.float32
BF16 = jnp.bfloat16


def layer_norm(resid, gain_f):
    resid_f = resid.astype(F32)
    row_mean = jnp.mean(resid_f, axis=-1, keepdims=True)
    centred = resid_f - row_mean
    row_var = jnp.mean(centred * centred, axis=-1, keepdims=True)
    return (centred * lax.rsqrt(row_var + NORM_EPS) * gain_f).astype(BF16)


def greet(partner):
    barrier = pltpu.get_barrier_semaphore()
    pl.semaphore_signal(barrier, inc=1, device_id={"tp": partner}, device_id_type=pl.DeviceIdType.MESH)
    pl.semaphore_wait(barrier, 1)


def other_core():
    rank = lax.axis_index("tp")
    return rank + 1 - 2 * lax.rem(rank, 2)


def up_kernel(virt, virt_next, own, far, w, a, b, gains, hid_top, hid_low, y_next, h_next, h, cand, gbuf, wbuf, wsem, lsem, ssem, rsem):
    j = pl.program_id(0)
    tiles = w.shape[3] // TILE
    tok = own.shape[0]
    partner = other_core()
    stage = lax.axis_index("pp")
    v = virt[0] + (virt[1] - virt[0]) * stage

    def weights(i, slot):
        cols = pl.ds(pl.multiple_of(i * TILE, TILE), TILE)
        return pltpu.make_async_copy(w.at[v, 0, :, cols], wbuf.at[slot], wsem.at[slot])

    def send(k):
        src = own if k == 0 else far
        return pltpu.make_async_remote_copy(
            src_ref=src, dst_ref=h.at[pl.ds((2 + k) * tok, tok)], send_sem=ssem.at[k], recv_sem=rsem.at[k],
            device_id={"tp": partner}, device_id_type=pl.DeviceIdType.MESH)

    def local(k):
        src = own if k == 0 else far
        return pltpu.make_async_copy(src, h.at[pl.ds(k * tok, tok)], lsem.at[k])

    side = [
        pltpu.make_async_copy(a, cand.at[0], lsem.at[2]),
        pltpu.make_async_copy(b, cand.at[1], lsem.at[3]),
        pltpu.make_async_copy(gains, gbuf, lsem.at[4]),
    ]
    part = tok // tiles

    def norm_rows():
        span = pl.ds(pl.multiple_of(jnp.minimum(j, tiles - 1) * part, part), part)
        y = jnp.where(stage == 0, cand[0, span], cand[1, span])
        y_next[...] = y
        g0, g1 = gbuf[virt_next[0]].astype(F32), gbuf[virt_next[1]].astype(F32)
        h_next[...] = layer_norm(y, jnp.where(stage == 0, g0, g1))

    def project(rows, slot):
        return jax.nn.gelu(jnp.dot(h[rows], wbuf[slot], preferred_element_type=F32)).astype(BF16)

    def fetch_next():
        @pl.when(j + 1 < tiles)
        def _():
            weights(j + 1, lax.rem(j + 1, SLOTS)).start()

    top, low = pl.ds(0, 2 * tok), pl.ds(2 * tok, 2 * tok)

    @pl.when(j == 0)
    def _():
        weights(0, 0).start()
        for k in range(2):
            local(k).start()
        greet(partner)
        for k in range(2):
            send(k).start()
        for copy in side:
            copy.start()
        for k in range(2):
            local(k).wait()
        weights(0, 0).wait()
        fetch_next()
        hid_top[...] = project(top, 0)
        for copy in side:
            copy.wait()
        norm_rows()

    @pl.when(j == 1)
    def _():
        for k in range(2):
            send(k).wait_recv()

    @pl.when((j > 0) & (j < tiles))
    def _():
        slot = lax.rem(j, SLOTS)
        weights(j, slot).wait()
        fetch_next()
        hid_top[...] = project(top, slot)
        norm_rows()
        hid_low[...] = project(low, lax.rem(j + SLOTS - 1, SLOTS))

    @pl.when(j == tiles)
    def _():
        hid_low[...] = project(low, (tiles - 1) % SLOTS)
        for k in range(2):
            send(k).wait_send()


def up_project(ids, virt, virt_next, own, far, w, a, b, gains):
    tok, dim, width = own.shape[0], w.shape[2], w.shape[3]
    rows = 4 * tok
    tiles = width // TILE
    part = tok // tiles
    any_spec = pl.BlockSpec(memory_space=pl.ANY)
    row_spec = pl.BlockSpec((part, dim), lambda j: (jnp.minimum(j, tiles - 1), 0))
    return pl.pallas_call(
        functools.partial(up_kernel, virt, virt_next),
        out_shape=[
            jax.ShapeDtypeStruct((2 * tok, width), BF16),
            jax.ShapeDtypeStruct((2 * tok, width), BF16),
            jax.ShapeDtypeStruct((tok, dim), BF16),
            jax.ShapeDtypeStruct((tok, dim), BF16),
        ],
        grid=(tiles + 1,),
        in_specs=[any_spec] * 6,
        out_specs=[
            pl.BlockSpec((2 * tok, TILE), lambda j: (0, jnp.minimum(j, tiles - 1))),
            pl.BlockSpec((2 * tok, TILE), lambda j: (0, jnp.maximum(j - 1, 0))),
            row_spec,
            row_spec,
        ],
        scratch_shapes=[
            pltpu.VMEM((rows, dim), BF16),
            pltpu.VMEM((2, tok, dim), BF16),
            pltpu.VMEM((2, 1, dim), BF16),
            pltpu.VMEM((SLOTS, dim, TILE), BF16),
            pltpu.SemaphoreType.DMA((SLOTS,)),
            pltpu.SemaphoreType.DMA((5,)),
            pltpu.SemaphoreType.DMA((2,)),
            pltpu.SemaphoreType.DMA((2,)),
        ],
        compiler_params=pltpu.CompilerParams(
            vmem_limit_bytes=34 * 2**20, has_side_effects=True, collective_id=ids.setdefault(("up", virt, virt_next), len(ids))),
        cost_estimate=pl.CostEstimate(flops=2 * rows * dim * width, bytes_accessed=40 * 2**20, transcendentals=rows * width),
        name="up_project",
    )(own, far, w, a, b, gains)


def down_kernel(virt, act_top, act_low, w, near, away, act, kbuf, sbuf, rbuf, wbuf, wsem, asem, ssem, rsem):
    j = pl.program_id(0)
    tiles = w.shape[3] // TILE
    tok = near.shape[0]
    partner = other_core()
    v = virt[0] + (virt[1] - virt[0]) * lax.axis_index("pp")

    def weights(i, slot):
        cols = pl.ds(pl.multiple_of(i * TILE, TILE), TILE)
        return pltpu.make_async_copy(w.at[v, 0, :, cols], wbuf.at[slot], wsem.at[slot])

    def send(i):
        return pltpu.make_async_remote_copy(
            src_ref=sbuf.at[i], dst_ref=rbuf.at[i], send_sem=ssem.at[i], recv_sem=rsem.at[i],
            device_id={"tp": partner}, device_id_type=pl.DeviceIdType.MESH)

    def combine(i):
        total = (kbuf[i].astype(F32) + rbuf[i].astype(F32)).astype(BF16)
        near[...] = total[:tok]
        away[...] = total[tok:]

    def multiply(i, slot):
        sbuf[i] = jnp.dot(act[1], wbuf[slot], preferred_element_type=F32).astype(BF16)
        kbuf[i] = jnp.dot(act[0], wbuf[slot], preferred_element_type=F32).astype(BF16)

    def fetch_next():
        @pl.when(j + 1 < tiles)
        def _():
            weights(j + 1, lax.rem(j + 1, SLOTS)).start()

    @pl.when(j == 0)
    def _():
        weights(0, 0).start()
        load = [pltpu.make_async_copy(src, act.at[k], asem.at[k]) for k, src in enumerate((act_top, act_low))]
        for copy in load:
            copy.start()
        greet(partner)
        for copy in load:
            copy.wait()

    @pl.when(j < 2)
    def _():
        slot = lax.rem(j, SLOTS)
        weights(j, slot).wait()
        fetch_next()
        multiply(j, slot)

    @pl.when((j >= 2) & (j < tiles))
    def _():
        slot = lax.rem(j, SLOTS)
        weights(j, slot).wait()
        fetch_next()
        send(j - 2).wait_recv()
        combine(j - 2)
        multiply(j, slot)

    @pl.when(j < tiles)
    def _():
        send(j).start()

    @pl.when(j >= tiles)
    def _():
        send(j - 2).wait_recv()
        combine(j - 2)

    @pl.when(j == tiles + 1)
    def _():
        for i in range(tiles):
            send(i).wait_send()


def down_project(ids, virt, top, low, w):
    tok, width, dim = top.shape[0] // 2, w.shape[2], w.shape[3]
    rows = 4 * tok
    tiles = dim // TILE
    out_spec = pl.BlockSpec((tok, TILE), lambda j: (0, jnp.maximum(j - 2, 0)))
    return pl.pallas_call(
        functools.partial(down_kernel, virt),
        out_shape=[jax.ShapeDtypeStruct((tok, dim), BF16)] * 2,
        grid=(tiles + 2,),
        in_specs=[pl.BlockSpec(memory_space=pl.ANY)] * 3,
        out_specs=[out_spec, out_spec],
        scratch_shapes=[
            pltpu.VMEM((2, 2 * tok, width), BF16),
            pltpu.VMEM((tiles, 2 * tok, TILE), BF16),
            pltpu.VMEM((tiles, 2 * tok, TILE), BF16),
            pltpu.VMEM((tiles, 2 * tok, TILE), BF16),
            pltpu.VMEM((SLOTS, width, TILE), BF16),
            pltpu.SemaphoreType.DMA((SLOTS,)),
            pltpu.SemaphoreType.DMA((2,)),
            pltpu.SemaphoreType.DMA((tiles,)),
            pltpu.SemaphoreType.DMA((tiles,)),
        ],
        compiler_params=pltpu.CompilerParams(
            vmem_limit_bytes=34 * 2**20, has_side_effects=True, collective_id=ids.setdefault(("down", virt), len(ids))),
        cost_estimate=pl.CostEstimate(flops=2 * rows * dim * width, bytes_accessed=40 * 2**20, transcendentals=0),
        name="down_project",
    )(top, low, w)


def solution(mesh):
    stages = mesh.shape["pp"]
    ranks = mesh.shape["tp"]
    assert stages == 2 and ranks == 4
    chip_perm = [(r, r ^ 2) for r in range(ranks)]
    stage_perm = [(0, 1), (1, 0)]
    ids = {}

    def per_device(x_loc, gain_loc, w_in_loc, w_out_loc):
        micro = x_loc.shape[0]
        items = 2 * micro
        ticks = items + LAG
        first = lax.axis_index("pp") == 0

        def virt(t):
            return min(t, items - 1) // micro, min(max(t - LAG, 0), items - 1) // micro

        shard, norm, far, other, near, new, recv = {}, {}, {}, {}, {}, {}, {}

        def sources(t):
            in0 = x_loc[t] if t < micro else recv.get(t - micro + LAG)
            in1 = recv.get(t - LAG)
            a = in1 if in0 is None else in0
            return a, (in0 if in1 is None else in1)

        def gather(t):
            if t < ticks:
                far[t] = lax.ppermute(norm[t], "tp", chip_perm)

        def finish(t):
            total = near[t].astype(F32) + other[t].astype(F32)
            return (shard[t].astype(F32) + total).astype(BF16)

        def tie(main, extras):
            keys = [(d, k) for d, k in extras if k in d]
            vals = lax.optimization_barrier((main, *[d[k] for d, k in keys]))
            for (d, k), val in zip(keys, vals[1:]):
                d[k] = val
            return vals[0]

        shard[0] = x_loc[0]
        norm[0] = layer_norm(shard[0], jnp.where(first, gain_loc[virt(0)[0], 0], gain_loc[virt(0)[1], 0]).astype(F32))
        gather(0)
        for t in range(ticks):
            after = min(t + 1, ticks - 1)
            a, b = sources(after)
            top, low, y_next, h_next = up_project(ids, virt(t), virt(after), norm[t], far[t], w_in_loc, a, b, gain_loc)
            if t + 1 < ticks:
                shard[t + 1], norm[t + 1] = y_next, h_next
            top = tie(top, [(other, t - 1)])
            if t >= 1:
                new[t - 1] = finish(t - 1)
                recv[t - 1] = lax.ppermute(new[t - 1], "pp", stage_perm)
            gather(t + 1)
            near[t], away = down_project(ids, virt(t), top, low, w_out_loc)
            away = tie(away, [(recv, t - 1), (far, t + 1)])
            other[t] = lax.ppermute(away, "tp", chip_perm)
        new[ticks - 1] = finish(ticks - 1)

        half = micro // stages
        outs = [jnp.where(first, recv[micro + k + LAG], new[micro + half + k + LAG]) for k in range(half)]
        return jnp.stack(outs, axis=0)

    return jax.shard_map(per_device, mesh=mesh, in_specs=(P("dp", "tp", None), P(None, "pp", None), P(None, "pp", None, "tp"), P(None, "pp", "tp", None)), out_specs=P(("dp", "pp"), "tp", None), check_vma=False)
```

```python
import functools

import jax
import jax.numpy as jnp
from jax import lax
from jax.experimental import pallas as pl
from jax.experimental.pallas import tpu as pltpu
from jax.sharding import PartitionSpec as P


NORM_EPS = 1e-5
LAG = 3
TILE = 512
SLOTS = 3
F32 = jnp.float32
BF16 = jnp.bfloat16


def layer_norm(resid, gain_f):
    resid_f = resid.astype(F32)
    row_mean = jnp.mean(resid_f, axis=-1, keepdims=True)
    centred = resid_f - row_mean
    row_var = jnp.mean(centred * centred, axis=-1, keepdims=True)
    return (centred * lax.rsqrt(row_var + NORM_EPS) * gain_f).astype(BF16)


def greet(partner):
    barrier = pltpu.get_barrier_semaphore()
    pl.semaphore_signal(barrier, inc=1, device_id={"tp": partner}, device_id_type=pl.DeviceIdType.MESH)
    pl.semaphore_wait(barrier, 1)


def gelu(x):
    half = 0.5 * x
    inner = x * (0.7978845608028654 + 0.035677408136300125 * (x * x))
    return half + half * jnp.tanh(inner)


def other_core():
    rank = lax.axis_index("tp")
    return rank + 1 - 2 * lax.rem(rank, 2)


def up_kernel(virt, virt_next, own, far, w, a, b, gains, hid_top, hid_low, y_next, h_next, h, cand, gbuf, wbuf, wsem, lsem, ssem, rsem):
    j = pl.program_id(0)
    tiles = w.shape[3] // TILE
    tok = own.shape[0]
    partner = other_core()
    stage = lax.axis_index("pp")
    v = virt[0] + (virt[1] - virt[0]) * stage

    def weights(i, slot):
        cols = pl.ds(pl.multiple_of(i * TILE, TILE), TILE)
        return pltpu.make_async_copy(w.at[v, 0, :, cols], wbuf.at[slot], wsem.at[slot])

    def send(k):
        src = own if k == 0 else far
        return pltpu.make_async_remote_copy(
            src_ref=src, dst_ref=h.at[pl.ds((2 + k) * tok, tok)], send_sem=ssem.at[k], recv_sem=rsem.at[k],
            device_id={"tp": partner}, device_id_type=pl.DeviceIdType.MESH)

    def local(k):
        src = own if k == 0 else far
        return pltpu.make_async_copy(src, h.at[pl.ds(k * tok, tok)], lsem.at[k])

    side = [
        pltpu.make_async_copy(a, cand.at[0], lsem.at[2]),
        pltpu.make_async_copy(b, cand.at[1], lsem.at[3]),
        pltpu.make_async_copy(gains, gbuf, lsem.at[4]),
    ]
    part = tok // tiles

    def norm_rows():
        span = pl.ds(pl.multiple_of(jnp.minimum(j, tiles - 1) * part, part), part)
        y = jnp.where(stage == 0, cand[0, span], cand[1, span])
        y_next[...] = y
        g0, g1 = gbuf[virt_next[0]].astype(F32), gbuf[virt_next[1]].astype(F32)
        h_next[...] = layer_norm(y, jnp.where(stage == 0, g0, g1))

    def project(rows, slot):
        return gelu(jnp.dot(h[rows], wbuf[slot], preferred_element_type=F32)).astype(BF16)

    def fetch_next():
        @pl.when(j + 1 < tiles)
        def _():
            weights(j + 1, lax.rem(j + 1, SLOTS)).start()

    top, low = pl.ds(0, 2 * tok), pl.ds(2 * tok, 2 * tok)

    @pl.when(j == 0)
    def _():
        weights(0, 0).start()
        for k in range(2):
            local(k).start()
        greet(partner)
        for k in range(2):
            send(k).start()
        for copy in side:
            copy.start()
        for k in range(2):
            local(k).wait()
        weights(0, 0).wait()
        fetch_next()
        hid_top[...] = project(top, 0)
        for copy in side:
            copy.wait()
        norm_rows()

    @pl.when(j == 1)
    def _():
        for k in range(2):
            send(k).wait_recv()

    @pl.when((j > 0) & (j < tiles))
    def _():
        slot = lax.rem(j, SLOTS)
        weights(j, slot).wait()
        fetch_next()
        hid_top[...] = project(top, slot)
        norm_rows()
        hid_low[...] = project(low, lax.rem(j + SLOTS - 1, SLOTS))

    @pl.when(j == tiles)
    def _():
        hid_low[...] = project(low, (tiles - 1) % SLOTS)
        for k in range(2):
            send(k).wait_send()


def up_project(ids, virt, virt_next, own, far, w, a, b, gains):
    tok, dim, width = own.shape[0], w.shape[2], w.shape[3]
    rows = 4 * tok
    tiles = width // TILE
    part = tok // tiles
    any_spec = pl.BlockSpec(memory_space=pl.ANY)
    row_spec = pl.BlockSpec((part, dim), lambda j: (jnp.minimum(j, tiles - 1), 0))
    return pl.pallas_call(
        functools.partial(up_kernel, virt, virt_next),
        out_shape=[
            jax.ShapeDtypeStruct((2 * tok, width), BF16),
            jax.ShapeDtypeStruct((2 * tok, width), BF16),
            jax.ShapeDtypeStruct((tok, dim), BF16),
            jax.ShapeDtypeStruct((tok, dim), BF16),
        ],
        grid=(tiles + 1,),
        in_specs=[any_spec] * 6,
        out_specs=[
            pl.BlockSpec((2 * tok, TILE), lambda j: (0, jnp.minimum(j, tiles - 1))),
            pl.BlockSpec((2 * tok, TILE), lambda j: (0, jnp.maximum(j - 1, 0))),
            row_spec,
            row_spec,
        ],
        scratch_shapes=[
            pltpu.VMEM((rows, dim), BF16),
            pltpu.VMEM((2, tok, dim), BF16),
            pltpu.VMEM((2, 1, dim), BF16),
            pltpu.VMEM((SLOTS, dim, TILE), BF16),
            pltpu.SemaphoreType.DMA((SLOTS,)),
            pltpu.SemaphoreType.DMA((5,)),
            pltpu.SemaphoreType.DMA((2,)),
            pltpu.SemaphoreType.DMA((2,)),
        ],
        compiler_params=pltpu.CompilerParams(
            vmem_limit_bytes=34 * 2**20, has_side_effects=True, collective_id=ids.setdefault(("up", virt, virt_next), len(ids))),
        cost_estimate=pl.CostEstimate(flops=2 * rows * dim * width, bytes_accessed=40 * 2**20, transcendentals=rows * width),
        name="up_project",
    )(own, far, w, a, b, gains)


def down_kernel(virt, base, tiles, act_top, act_low, w, near, away, act, kbuf, sbuf, rbuf, wbuf, wsem, asem, ssem, rsem):
    j = pl.program_id(0)
    tok = near.shape[0]
    partner = other_core()
    v = virt[0] + (virt[1] - virt[0]) * lax.axis_index("pp")

    def weights(i, slot):
        cols = pl.ds(pl.multiple_of((base + i) * TILE, TILE), TILE)
        return pltpu.make_async_copy(w.at[v, 0, :, cols], wbuf.at[slot], wsem.at[slot])

    def send(i):
        return pltpu.make_async_remote_copy(
            src_ref=sbuf.at[i], dst_ref=rbuf.at[i], send_sem=ssem.at[i], recv_sem=rsem.at[i],
            device_id={"tp": partner}, device_id_type=pl.DeviceIdType.MESH)

    def combine(i):
        total = (kbuf[i].astype(F32) + rbuf[i].astype(F32)).astype(BF16)
        near[...] = total[:tok]
        away[...] = total[tok:]

    def multiply(i, slot):
        sbuf[i] = jnp.dot(act[1], wbuf[slot], preferred_element_type=F32).astype(BF16)
        kbuf[i] = jnp.dot(act[0], wbuf[slot], preferred_element_type=F32).astype(BF16)

    def fetch_next():
        @pl.when(j + 1 < tiles)
        def _():
            weights(j + 1, lax.rem(j + 1, SLOTS)).start()

    @pl.when(j == 0)
    def _():
        weights(0, 0).start()
        load = [pltpu.make_async_copy(src, act.at[k], asem.at[k]) for k, src in enumerate((act_top, act_low))]
        for copy in load:
            copy.start()
        greet(partner)
        for copy in load:
            copy.wait()

    @pl.when(j < 2)
    def _():
        slot = lax.rem(j, SLOTS)
        weights(j, slot).wait()
        fetch_next()
        multiply(j, slot)

    @pl.when((j >= 2) & (j < tiles))
    def _():
        slot = lax.rem(j, SLOTS)
        weights(j, slot).wait()
        fetch_next()
        send(j - 2).wait_recv()
        combine(j - 2)
        multiply(j, slot)

    @pl.when(j < tiles)
    def _():
        send(j).start()

    @pl.when(j >= tiles)
    def _():
        send(j - 2).wait_recv()
        combine(j - 2)

    @pl.when(j == tiles + 1)
    def _():
        for i in range(tiles):
            send(i).wait_send()


def down_project(ids, virt, top, low, w, piece=0, pieces=1):
    tok, width, dim = top.shape[0] // 2, w.shape[2], w.shape[3]
    rows = 4 * tok
    tiles = dim // TILE // pieces
    out_spec = pl.BlockSpec((tok, TILE), lambda j: (0, jnp.maximum(j - 2, 0)))
    return pl.pallas_call(
        functools.partial(down_kernel, virt, piece * tiles, tiles),
        out_shape=[jax.ShapeDtypeStruct((tok, tiles * TILE), BF16)] * 2,
        grid=(tiles + 2,),
        in_specs=[pl.BlockSpec(memory_space=pl.ANY)] * 3,
        out_specs=[out_spec, out_spec],
        scratch_shapes=[
            pltpu.VMEM((2, 2 * tok, width), BF16),
            pltpu.VMEM((tiles, 2 * tok, TILE), BF16),
            pltpu.VMEM((tiles, 2 * tok, TILE), BF16),
            pltpu.VMEM((tiles, 2 * tok, TILE), BF16),
            pltpu.VMEM((SLOTS, width, TILE), BF16),
            pltpu.SemaphoreType.DMA((SLOTS,)),
            pltpu.SemaphoreType.DMA((2,)),
            pltpu.SemaphoreType.DMA((tiles,)),
            pltpu.SemaphoreType.DMA((tiles,)),
        ],
        compiler_params=pltpu.CompilerParams(
            vmem_limit_bytes=34 * 2**20, has_side_effects=True, collective_id=ids.setdefault(("down", virt, piece, pieces), len(ids))),
        cost_estimate=pl.CostEstimate(flops=2 * rows * dim * width // pieces, bytes_accessed=40 * 2**20, transcendentals=0),
        name="down_project",
    )(top, low, w)


def solution(mesh):
    stages = mesh.shape["pp"]
    ranks = mesh.shape["tp"]
    assert stages == 2 and ranks == 4
    chip_perm = [(r, r ^ 2) for r in range(ranks)]
    stage_perm = [(0, 1), (1, 0)]
    ids = {}

    def per_device(x_loc, gain_loc, w_in_loc, w_out_loc):
        micro = x_loc.shape[0]
        items = 2 * micro
        ticks = items + LAG
        first = lax.axis_index("pp") == 0

        def virt(t):
            return min(t, items - 1) // micro, min(max(t - LAG, 0), items - 1) // micro

        shard, norm, far, other, near, new, recv = {}, {}, {}, {}, {}, {}, {}

        def sources(t):
            in0 = x_loc[t] if t < micro else recv.get(t - micro + LAG)
            in1 = recv.get(t - LAG)
            a = in1 if in0 is None else in0
            return a, (in0 if in1 is None else in1)

        def gather(t):
            if t < ticks:
                far[t] = lax.ppermute(norm[t], "tp", chip_perm)

        def finish(t):
            total = near[t].astype(F32) + other[t].astype(F32)
            return (shard[t].astype(F32) + total).astype(BF16)

        def tie(main, extras):
            keys = [(d, k) for d, k in extras if k in d]
            vals = lax.optimization_barrier((main, *[d[k] for d, k in keys]))
            for (d, k), val in zip(keys, vals[1:]):
                d[k] = val
            return vals[0]

        shard[0] = x_loc[0]
        norm[0] = layer_norm(shard[0], jnp.where(first, gain_loc[virt(0)[0], 0], gain_loc[virt(0)[1], 0]).astype(F32))
        gather(0)
        for t in range(ticks):
            after = min(t + 1, ticks - 1)
            a, b = sources(after)
            top, low, y_next, h_next = up_project(ids, virt(t), virt(after), norm[t], far[t], w_in_loc, a, b, gain_loc)
            if t + 1 < ticks:
                shard[t + 1], norm[t + 1] = y_next, h_next
            top = tie(top, [(other, t - 1)])
            if t >= 1:
                new[t - 1] = finish(t - 1)
                recv[t - 1] = lax.ppermute(new[t - 1], "pp", stage_perm)
            gather(t + 1)
            if t == ticks - 1:
                break
            near[t], away = down_project(ids, virt(t), top, low, w_out_loc)
            away = tie(away, [(recv, t - 1), (far, t + 1)])
            other[t] = lax.ppermute(away, "tp", chip_perm)
        last, pieces = ticks - 1, 2
        wide = shard[last].shape[1] // pieces
        done = []
        for piece in range(pieces):
            kept, away = down_project(ids, virt(last), top, low, w_out_loc, piece, pieces)
            came = lax.ppermute(away, "tp", chip_perm)
            old = shard[last][:, piece * wide:(piece + 1) * wide]
            done.append((old.astype(F32) + (kept.astype(F32) + came.astype(F32))).astype(BF16))
        new[last] = jnp.concatenate(done, axis=1)

        half = micro // stages
        outs = [jnp.where(first, recv[micro + k + LAG], new[micro + half + k + LAG]) for k in range(half)]
        return jnp.stack(outs, axis=0)

    return jax.shard_map(per_device, mesh=mesh, in_specs=(P("dp", "tp", None), P(None, "pp", None), P(None, "pp", None, "tp"), P(None, "pp", "tp", None)), out_specs=P(("dp", "pp"), "tp", None), check_vma=False)
```
